32 devices in a mesh: row: 4 (over z), col: 2 (over y), depth: 4 (over x, core).
Axes of the slice: x: 2, y: 2, z: 4, core: 2. Of those that a mesh axis runs over, the one named last changes fastest.
Arguments:
- a21_leaf: float32 [4, 4096, 2048], P('depth', 'row', 'col'), may hold values from -1.2 to 1.2
- a12_leaf: float32 [4, 2048, 4096], P('depth', 'row', 'col'), may hold values from -1.2 to 1.2
- uinv_leaf: float32 [4, 2048, 2048], P('depth', None, 'col'), may hold values from -0.2 to 1.5, as said below
- linv_leaf: float32 [4, 2048, 2048], P('depth', 'row'), may hold values from -0.2 to 1.5, as said below
- live: int32 [4], P('depth'), may hold values from 16 to 32
- row_map: int32 [4, 32], P('depth', 'row'), may hold values from 0 to 63, as said below
- col_map: int32 [4, 32], P('depth', 'col'), may hold values from 0 to 63, as said below
- a22_anc: float32 [8192, 8192], P(('row', 'depth'), 'col'), may hold values from -6 to 6
- a21_anc: float32 [8192, 2048], P(('row', 'depth'), 'col'), may hold values from -1.2 to 1.2
- a12_anc: float32 [2048, 8192], P(('row', 'depth'), 'col'), may hold values from -1.2 to 1.2
- uinv_anc: float32 [2048, 2048], P(None, 'col'), may hold values from -0.2 to 1.5, as said below
- linv_anc: float32 [2048, 2048], P(('row', 'depth')), may hold values from -0.2 to 1.5, as said below
Outputs:
- leaf_lower: float32 [4, 4096, 2048], P('depth', 'row', 'col')
- leaf_upper: float32 [4, 2048, 4096], P('depth', 'row', 'col')
- anc_lower: float32 [8192, 2048], P(('row', 'depth'), 'col')
- anc_upper: float32 [2048, 8192], P(('row', 'depth'), 'col')
- anc_schur: float32 [8192, 8192], P(('row', 'depth'), 'col')
The draws below stay inside these ranges and needn't reach their ends.
Inputs may be any that keep to these rules, and one draw needn't show every extreme that they name: `uinv_leaf`: upper triangular: zero below the diagonal, diagonal between 0.5 and 1.5. `linv_leaf`: lower triangular: zero above the diagonal, diagonal between 0.5 and 1.5. `uinv_anc`: upper triangular: zero below the diagonal, diagonal between 0.5 and 1.5. `linv_anc`: lower triangular: zero above the diagonal, diagonal between 0.5 and 1.5. `row_map`: within one replica the entries are distinct. Leaf block row i lies in the k-th of 4 equal ranges of leaf block rows, and its target lies in the k-th of 4 equal ranges of the 64 ancestor block rows. `col_map`: within one replica the entries are distinct. Leaf block column j lies in the k-th of 2 equal ranges of leaf block columns, and its target lies in the k-th of 2 equal ranges of the 64 ancestor block columns.
All inputs are finite; a program needn't handle non-finite values.
Results may differ from the reference program's by a relative error of at most 0.0001.
Values sent between devices are 32-bit elements; how exact they have to be, the bound alone decides.
A program may use at most 256 MiB of HBM per device.

```python
from functools import partial
import jax
import jax.numpy as jnp
from jax import lax

NB = 128
WL = 2048
WA = 2048
R = 4096
RA = 8192
N_ROW = 4
N_COL = 2
N_DEPTH = 4


def triangle(subkey, order, upper):
    first, second = jax.random.split(subkey)
    spread = jnp.clip(jax.random.normal(first, (order, order), jnp.float32) * (0.5 / order ** 0.5), -0.2, 0.2)
    diagonal = jax.random.uniform(second, (order,), jnp.float32, 0.5, 1.5)
    if upper:
        strict = jnp.triu(spread, 1)
    else:
        strict = jnp.tril(spread, -1)
    return strict + jnp.diag(diagonal)


def draw_uinv_leaf(key, part):
    subkeys = jax.random.split(jax.random.fold_in(key, 11), N_DEPTH)
    return jax.vmap(partial(triangle, order=WL, upper=True))(subkeys)


def draw_linv_leaf(key, part):
    subkeys = jax.random.split(jax.random.fold_in(key, 12), N_DEPTH)
    return jax.vmap(partial(triangle, order=WL, upper=False))(subkeys)


def draw_uinv_anc(key, part):
    return triangle(jax.random.fold_in(key, 13), WA, True)


def draw_linv_anc(key, part):
    return triangle(jax.random.fold_in(key, 14), WA, False)


def pick_targets(subkey, per_leaf, per_anc):
    return jax.random.permutation(subkey, per_anc)[:per_leaf]


def owner_map(key, groups):
    per_leaf = R // (NB * groups)
    per_anc = RA // (NB * groups)
    subkeys = jax.random.split(key, N_DEPTH * groups)
    chosen = jax.vmap(partial(pick_targets, per_leaf=per_leaf, per_anc=per_anc))(subkeys)
    base = jnp.arange(N_DEPTH * groups) % groups * per_anc
    return (chosen + base[:, None]).reshape(N_DEPTH, groups * per_leaf).astype(jnp.int32)


def draw_row_map(key, part):
    return owner_map(jax.random.fold_in(key, 16), N_ROW)


def draw_col_map(key, part):
    return owner_map(jax.random.fold_in(key, 17), N_COL)


def place_ends(array, own_key, smallest, high):
    index_at = [jax.random.randint(jax.random.fold_in(own_key, axis), (), 0, length) for axis, length in enumerate(array.shape)]
    longest = array.shape.index(max(array.shape))
    beside = index_at[:longest] + [(index_at[longest] + 1) % array.shape[longest]] + index_at[longest + 1:]
    return array.at[tuple(index_at)].set(smallest).at[tuple(beside)].set(high)


def levels(own_key, extent, shards, least, top_value):
    loudness, own = 1.0, jax.random.fold_in(own_key, 6)
    for axis_at, parts in shards:
        draws = jnp.exp(jax.random.uniform(jax.random.fold_in(own, axis_at), (parts,), jnp.float32, least / len(shards), top_value / len(shards)))
        loudness = loudness * jnp.repeat(draws, extent[axis_at] // parts).reshape([-1 if axis == axis_at else 1 for axis in range(len(extent))])
    return loudness


def gaussian(stream_key, shape, scale, most, pieces=(), kind=jnp.bfloat16):
    drawn = scale * jax.random.normal(stream_key, shape, jnp.float32)
    if pieces:
        drawn = drawn * levels(stream_key, shape, pieces, -0.22, 0.18)
    return jnp.clip(drawn, -most, most).astype(kind)


def setup_inputs(seed: int = 0) -> dict:
    seeds = jax.random.split(jax.random.key(seed), 13)
    a21_leaf = gaussian(seeds[0], (N_DEPTH, R, WL), 0.18, 1.2, ((0, 4), (1, 4), (2, 2)), jnp.float32)
    a12_leaf = gaussian(seeds[1], (N_DEPTH, WL, R), 0.18, 1.2, ((0, 4), (1, 4), (2, 2)), jnp.float32)
    uinv_leaf = draw_uinv_leaf(jax.random.fold_in(seeds[12], 71), 0)
    linv_leaf = draw_linv_leaf(jax.random.fold_in(seeds[12], 71), 0)
    live = place_ends(jax.random.randint(seeds[4], (N_DEPTH,), R // NB // 2, R // NB + 1), jax.random.fold_in(seeds[4], 1), R // NB // 2, (R // NB + 1) - 1).astype(jnp.int32)
    row_map = draw_row_map(jax.random.fold_in(seeds[12], 71), 0)
    col_map = draw_col_map(jax.random.fold_in(seeds[12], 71), 0)
    a22_anc = gaussian(seeds[7], (RA, RA), 1.0, 6.0, ((0, 16), (1, 2)), jnp.float32)
    a21_anc = gaussian(seeds[8], (RA, WA), 0.18, 1.2, ((0, 16), (1, 2)), jnp.float32)
    a12_anc = gaussian(seeds[9], (WA, RA), 0.18, 1.2, ((0, 16), (1, 2)), jnp.float32)
    uinv_anc = draw_uinv_anc(jax.random.fold_in(seeds[12], 71), 0)
    linv_anc = draw_linv_anc(jax.random.fold_in(seeds[12], 71), 0)
    return {"a21_leaf": a21_leaf, "a12_leaf": a12_leaf, "uinv_leaf": uinv_leaf, "linv_leaf": linv_leaf, "live": live, "row_map": row_map, "col_map": col_map, "a22_anc": a22_anc, "a21_anc": a21_anc, "a12_anc": a12_anc, "uinv_anc": uinv_anc, "linv_anc": linv_anc}


def product(left, right):
    return jnp.dot(left, right, precision=lax.Precision.HIGHEST, preferred_element_type=jnp.float32)


def reference(a21_leaf, a12_leaf, uinv_leaf, linv_leaf, live, row_map, col_map, a22_anc, a21_anc, a12_anc, uinv_anc, linv_anc):
    positions = jnp.arange(R, dtype=jnp.int32)
    block_ids = (positions // NB).astype(jnp.int32)
    offsets = (positions % NB).astype(jnp.int32)
    update = jnp.zeros((RA, RA), jnp.float32)
    lowers = []
    uppers = []
    for depth in range(N_DEPTH):
        keep = (block_ids < live[depth]).astype(jnp.float32)
        lower = product(a21_leaf[depth], uinv_leaf[depth]) * keep[:, None]
        upper = product(linv_leaf[depth], a12_leaf[depth]) * keep[None, :]
        schur = -product(lower, upper)
        rows = (row_map[depth][block_ids] * NB + offsets).astype(jnp.int32)
        cols = (col_map[depth][block_ids] * NB + offsets).astype(jnp.int32)
        update = update.at[rows[:, None], cols[None, :]].add(schur)
        lowers.append(lower)
        uppers.append(upper)
    leaf_lower = jnp.stack(lowers)
    leaf_upper = jnp.stack(uppers)
    anc_lower = product(a21_anc, uinv_anc)
    anc_upper = product(linv_anc, a12_anc)
    anc_schur = a22_anc + update - product(anc_lower, anc_upper)
    return leaf_lower, leaf_upper, anc_lower, anc_upper, anc_schur
```

```python
import functools

import jax
import jax.numpy as jnp
from jax import lax
from jax.experimental import pallas as pl
from jax.experimental.pallas import tpu as pltpu
from jax.sharding import PartitionSpec as P

NB = 128
CHUNKS = 2


def product(left, right):
    return jnp.dot(left, right, precision=lax.Precision.HIGH, preferred_element_type=jnp.float32)


def gather_cols(block):
    if lax.axis_size("col") != 2:
        return lax.all_gather(block, "col", axis=1, tiled=True)
    other = lax.ppermute(block, "col", [(0, 1), (1, 0)])
    first = lax.axis_index("col") == 0
    return jnp.concatenate(
        [jnp.where(first, block, other), jnp.where(first, other, block)], axis=1
    )


def own_columns(matrix):
    width = matrix.shape[1] // lax.axis_size("col")
    return lax.dynamic_slice_in_dim(matrix, lax.axis_index("col") * width, width, axis=1)


def chunk_count(columns):
    chunks = CHUNKS
    while columns % (chunks * NB):
        chunks -= 1
    return chunks


def after(value, earlier):
    return lax.optimization_barrier((value, earlier))[0]


def place_rows_kernel(source_ref, valid_ref, block_ref, out_ref):
    scale = valid_ref[pl.program_id(0)].astype(jnp.float32)
    out_ref[...] = block_ref[...] * scale


def place_rows(schur, source, valid):
    slots = source.shape[0]
    width = schur.shape[1]
    return pl.pallas_call(
        place_rows_kernel,
        out_shape=jax.ShapeDtypeStruct((slots * NB, width), jnp.float32),
        grid_spec=pltpu.PrefetchScalarGridSpec(
            num_scalar_prefetch=2,
            grid=(slots,),
            in_specs=[pl.BlockSpec((NB, width), lambda i, source, valid: (source[i], 0))],
            out_specs=pl.BlockSpec((NB, width), lambda i, source, valid: (i, 0)),
        ),
        cost_estimate=pl.CostEstimate(
            flops=slots * NB * width, bytes_accessed=8 * slots * NB * width, transcendentals=0
        ),
    )(source, valid, schur)


def add_columns_kernel(replicas, source_ref, valid_ref, *refs):
    step = pl.program_id(0)
    blocks, base_ref, out_ref = refs[:replicas], refs[replicas], refs[replicas + 1]
    total = base_ref[...]
    for k in range(replicas):
        scale = valid_ref[k, step].astype(jnp.float32)
        total = total - blocks[k][...] * scale
    out_ref[...] = total


def add_columns(base, parts, source, valid):
    replicas = len(parts)
    rows, columns = base.shape
    steps = columns // NB

    def pick(k):
        return pl.BlockSpec((rows, NB), lambda b, source, valid: (0, source[k, b]))

    plain = pl.BlockSpec((rows, NB), lambda b, source, valid: (0, b))
    return pl.pallas_call(
        functools.partial(add_columns_kernel, replicas),
        out_shape=jax.ShapeDtypeStruct(base.shape, jnp.float32),
        grid_spec=pltpu.PrefetchScalarGridSpec(
            num_scalar_prefetch=2,
            grid=(steps,),
            in_specs=[pick(k) for k in range(replicas)] + [plain],
            out_specs=plain,
        ),
        input_output_aliases={2 + replicas: 0},
        cost_estimate=pl.CostEstimate(
            flops=replicas * rows * columns, bytes_accessed=16 * rows * columns, transcendentals=0
        ),
    )(source, valid, *parts, base)


def inverse_map(targets, present, count):
    hit = (targets[:, None] == lax.iota(jnp.int32, count)[None, :]) & present[:, None]
    index = lax.iota(jnp.int32, targets.shape[0])[:, None]
    source = jnp.sum(jnp.where(hit, index, 0), axis=0).astype(jnp.int32)
    valid = jnp.any(hit, axis=0).astype(jnp.int32)
    return source, valid


def partner(index, k, count):
    if count & (count - 1) == 0:
        return index ^ k
    return (index + k) % count


def origin(index, k, count):
    if count & (count - 1) == 0:
        return index ^ k
    return (index + count - k) % count


def shards(
    a21_leaf,
    a12_leaf,
    uinv_leaf,
    linv_leaf,
    live,
    row_map,
    col_map,
    a22_anc,
    a21_anc,
    a12_anc,
    uinv_anc,
    linv_anc,
):
    replicas = lax.axis_size("depth")
    depth = lax.axis_index("depth")
    panel_left = a21_leaf[0]
    panel_top = a12_leaf[0]
    lower_inverse = linv_leaf[0]
    rows_here = panel_left.shape[0]
    cols_here = panel_top.shape[1]
    live_rows = live[0] * NB
    row_pos = lax.axis_index("row") * rows_here + lax.iota(jnp.int32, rows_here)
    col_pos = lax.axis_index("col") * cols_here + lax.iota(jnp.int32, cols_here)
    row_keep = (row_pos < live_rows).astype(jnp.float32)
    col_keep = (col_pos < live_rows).astype(jnp.float32)

    leaf_rows = rows_here // NB
    leaf_cols = cols_here // NB
    slots = a22_anc.shape[0] // NB
    anc_row_blocks = slots * replicas
    anc_col_blocks = a22_anc.shape[1] // NB
    row_local = row_map[0] - lax.axis_index("row") * anc_row_blocks
    always = jnp.ones((leaf_rows,), jnp.bool_)
    row_source, row_valid = inverse_map(row_local, always, anc_row_blocks)
    col_maps = lax.all_gather(col_map, "depth", axis=0, tiled=True)
    lives = lax.all_gather(live, "depth", axis=0, tiled=True)
    col_sources, col_valids = [], []
    for k in range(replicas):
        d = origin(depth, k, replicas)
        col_local = lax.dynamic_index_in_dim(col_maps, d, 0, keepdims=False)
        col_local = col_local - lax.axis_index("col") * anc_col_blocks
        leaf_block = lax.axis_index("col") * leaf_cols + lax.iota(jnp.int32, leaf_cols)
        present = leaf_block < lax.dynamic_index_in_dim(lives, d, 0, keepdims=False)
        source, valid = inverse_map(col_local, present, anc_col_blocks)
        col_sources.append(source)
        col_valids.append(valid)
    col_source = jnp.stack(col_sources)
    col_valid = jnp.stack(col_valids)

    chunks = chunk_count(cols_here)
    width = cols_here // chunks
    blocks = width // NB
    linv_own = after(own_columns(lower_inverse), (col_source, col_valid))
    linv_part = lax.all_gather(linv_own, "row", axis=0, tiled=True)
    leaf_lower = product(gather_cols(panel_left), uinv_leaf[0]) * row_keep[:, None]
    earlier = (linv_part, leaf_lower)
    left = None
    tops = []
    packs = []
    for q in range(chunks):
        piece = panel_top[:, q * width : (q + 1) * width]
        top = lax.all_gather(after(piece, earlier), "row", axis=0, tiled=True)
        tops.append(top)
        if q == 0:
            left = gather_cols(product(gather_cols(leaf_lower), linv_part))
        earlier = (top, left)
    linv_anc_own = after(own_columns(linv_anc), earlier)
    linv_anc_part = lax.all_gather(linv_anc_own, ("row", "depth"), axis=0, tiled=True)
    anc_lower = product(gather_cols(after(a21_anc, left)), uinv_anc)

    total = a22_anc
    uppers = []
    for q, top in enumerate(tops):
        schur = product(left, top)
        parts = []
        for k in range(replicas):
            begin = partner(depth, k, replicas) * slots
            packed = place_rows(
                schur,
                lax.dynamic_slice_in_dim(row_source, begin, slots),
                lax.dynamic_slice_in_dim(row_valid, begin, slots),
            )
            packs.append(packed)
            if k:
                pairs = [(d, partner(d, k, replicas)) for d in range(replicas)]
                packed = lax.ppermute(packed, "depth", pairs)
            parts.append(packed)
        keep = col_keep[q * width : (q + 1) * width]
        uppers.append(product(lower_inverse, top) * keep[None, :])
        inside = (col_source >= q * blocks) & (col_source < (q + 1) * blocks)
        local = jnp.clip(col_source - q * blocks, 0, blocks - 1)
        total = add_columns(total, parts, local, col_valid * inside.astype(jnp.int32))
    leaf_upper = jnp.concatenate(uppers, axis=1)

    anc_chunks = 1
    anc_width = a12_anc.shape[1] // anc_chunks
    earlier = (linv_anc_part, anc_lower, packs[-1])
    left_anc = None
    tops_anc = []
    for q in range(anc_chunks):
        piece = a12_anc[:, q * anc_width : (q + 1) * anc_width]
        top = lax.all_gather(after(piece, earlier), ("row", "depth"), axis=0, tiled=True)
        tops_anc.append(top)
        if q == 0:
            left_anc = gather_cols(product(gather_cols(anc_lower), linv_anc_part))
        earlier = (top, left_anc, total)

    anc_uppers, anc_schurs = [], []
    for q, top in enumerate(tops_anc):
        here = total[:, q * anc_width : (q + 1) * anc_width]
        anc_schurs.append(here - product(left_anc, top))
        anc_uppers.append(product(linv_anc, top))
    anc_upper = jnp.concatenate(anc_uppers, axis=1)
    anc_schur = jnp.concatenate(anc_schurs, axis=1)
    return (leaf_lower[None], leaf_upper[None], anc_lower, anc_upper, anc_schur)


def solution(mesh):
    in_specs = (
        P("depth", "row", "col"),
        P("depth", "row", "col"),
        P("depth", None, "col"),
        P("depth", "row", None),
        P("depth"),
        P("depth", "row"),
        P("depth", "col"),
        P(("row", "depth"), "col"),
        P(("row", "depth"), "col"),
        P(("row", "depth"), "col"),
        P(None, "col"),
        P(("row", "depth"), None),
    )
    out_specs = (
        P("depth", "row", "col"),
        P("depth", "row", "col"),
        P(("row", "depth"), "col"),
        P(("row", "depth"), "col"),
        P(("row", "depth"), "col"),
    )
    return jax.shard_map(shards, mesh=mesh, in_specs=in_specs, out_specs=out_specs, check_vma=False)
```

```python
import functools

import jax
import jax.numpy as jnp
from jax import lax
from jax.experimental import pallas as pl
from jax.experimental.pallas import tpu as pltpu
from jax.sharding import PartitionSpec as P

NB = 128
CHUNKS = 2


def product(left, right):
    return jnp.dot(left, right, precision=lax.Precision.HIGH, preferred_element_type=jnp.float32)


def gather_cols(block):
    if lax.axis_size("col") != 2:
        return lax.all_gather(block, "col", axis=1, tiled=True)
    other = lax.ppermute(block, "col", [(0, 1), (1, 0)])
    first = lax.axis_index("col") == 0
    return jnp.concatenate(
        [jnp.where(first, block, other), jnp.where(first, other, block)], axis=1
    )


def own_columns(matrix):
    width = matrix.shape[1] // lax.axis_size("col")
    return lax.dynamic_slice_in_dim(matrix, lax.axis_index("col") * width, width, axis=1)


def after(value, earlier):
    return lax.optimization_barrier((value, earlier))[0]


def place_rows_kernel(source_ref, valid_ref, block_ref, out_ref):
    scale = valid_ref[pl.program_id(0)].astype(jnp.float32)
    out_ref[...] = block_ref[...] * scale


def place_rows(schur, source, valid):
    slots = source.shape[0]
    width = schur.shape[1]
    return pl.pallas_call(
        place_rows_kernel,
        out_shape=jax.ShapeDtypeStruct((slots * NB, width), jnp.float32),
        grid_spec=pltpu.PrefetchScalarGridSpec(
            num_scalar_prefetch=2,
            grid=(slots,),
            in_specs=[pl.BlockSpec((NB, width), lambda i, source, valid: (source[i], 0))],
            out_specs=pl.BlockSpec((NB, width), lambda i, source, valid: (i, 0)),
        ),
        cost_estimate=pl.CostEstimate(
            flops=slots * NB * width, bytes_accessed=8 * slots * NB * width, transcendentals=0
        ),
    )(source, valid, schur)


def add_columns_kernel(replicas, source_ref, valid_ref, *refs):
    step = pl.program_id(0)
    blocks, base_ref, out_ref = refs[:replicas], refs[replicas], refs[replicas + 1]
    total = base_ref[...]
    for k in range(replicas):
        scale = valid_ref[k, step].astype(jnp.float32)
        total = total - blocks[k][...] * scale
    out_ref[...] = total


def add_columns(base, parts, source, valid):
    replicas = len(parts)
    rows, columns = base.shape
    steps = columns // NB

    def pick(k):
        return pl.BlockSpec((rows, NB), lambda b, source, valid: (0, source[k, b]))

    plain = pl.BlockSpec((rows, NB), lambda b, source, valid: (0, b))
    return pl.pallas_call(
        functools.partial(add_columns_kernel, replicas),
        out_shape=jax.ShapeDtypeStruct(base.shape, jnp.float32),
        grid_spec=pltpu.PrefetchScalarGridSpec(
            num_scalar_prefetch=2,
            grid=(steps,),
            in_specs=[pick(k) for k in range(replicas)] + [plain],
            out_specs=plain,
        ),
        input_output_aliases={2 + replicas: 0},
        cost_estimate=pl.CostEstimate(
            flops=replicas * rows * columns, bytes_accessed=16 * rows * columns, transcendentals=0
        ),
    )(source, valid, *parts, base)


def inverse_map(targets, present, count):
    hit = (targets[:, None] == lax.iota(jnp.int32, count)[None, :]) & present[:, None]
    index = lax.iota(jnp.int32, targets.shape[0])[:, None]
    source = jnp.sum(jnp.where(hit, index, 0), axis=0).astype(jnp.int32)
    valid = jnp.any(hit, axis=0).astype(jnp.int32)
    return source, valid


def partner(index, k, count):
    if count & (count - 1) == 0:
        return index ^ k
    return (index + k) % count


def origin(index, k, count):
    if count & (count - 1) == 0:
        return index ^ k
    return (index + count - k) % count


def shards(
    a21_leaf,
    a12_leaf,
    uinv_leaf,
    linv_leaf,
    live,
    row_map,
    col_map,
    a22_anc,
    a21_anc,
    a12_anc,
    uinv_anc,
    linv_anc,
):
    replicas = lax.axis_size("depth")
    depth = lax.axis_index("depth")
    panel_left = a21_leaf[0]
    panel_top = a12_leaf[0]
    lower_inverse = linv_leaf[0]
    rows_here = panel_left.shape[0]
    cols_here = panel_top.shape[1]
    live_rows = live[0] * NB
    row_pos = lax.axis_index("row") * rows_here + lax.iota(jnp.int32, rows_here)
    col_pos = lax.axis_index("col") * cols_here + lax.iota(jnp.int32, cols_here)
    row_keep = (row_pos < live_rows).astype(jnp.float32)
    col_keep = (col_pos < live_rows).astype(jnp.float32)

    leaf_rows = rows_here // NB
    leaf_cols = cols_here // NB
    slots = a22_anc.shape[0] // NB
    anc_row_blocks = slots * replicas
    anc_col_blocks = a22_anc.shape[1] // NB
    row_local = row_map[0] - lax.axis_index("row") * anc_row_blocks
    always = jnp.ones((leaf_rows,), jnp.bool_)
    row_source, row_valid = inverse_map(row_local, always, anc_row_blocks)
    col_maps = lax.all_gather(col_map, "depth", axis=0, tiled=True)
    lives = lax.all_gather(live, "depth", axis=0, tiled=True)
    col_sources, col_valids = [], []
    for k in range(replicas):
        d = origin(depth, k, replicas)
        col_local = lax.dynamic_index_in_dim(col_maps, d, 0, keepdims=False)
        col_local = col_local - lax.axis_index("col") * anc_col_blocks
        leaf_block = lax.axis_index("col") * leaf_cols + lax.iota(jnp.int32, leaf_cols)
        present = leaf_block < lax.dynamic_index_in_dim(lives, d, 0, keepdims=False)
        source, valid = inverse_map(col_local, present, anc_col_blocks)
        col_sources.append(source)
        col_valids.append(valid)
    col_source = jnp.stack(col_sources)
    col_valid = jnp.stack(col_valids)

    linv_part = lax.all_gather(own_columns(lower_inverse), "row", axis=0, tiled=True)
    linv_anc_part = lax.all_gather(
        own_columns(linv_anc), ("row", "depth"), axis=0, tiled=True
    )
    leaf_lower = product(gather_cols(panel_left), uinv_leaf[0]) * row_keep[:, None]
    anc_lower = product(gather_cols(a21_anc), uinv_anc)
    left = gather_cols(product(gather_cols(leaf_lower), linv_part))
    left_anc = gather_cols(product(gather_cols(anc_lower), linv_anc_part))

    top_anc = lax.all_gather(after(a12_anc, linv_part), ("row", "depth"), axis=0, tiled=True)
    anc_upper = product(linv_anc, top_anc)
    total = a22_anc - product(left_anc, top_anc)

    chunks = CHUNKS
    while cols_here % (chunks * NB):
        chunks -= 1
    width = cols_here // chunks
    blocks = width // NB
    uppers = []
    earlier = top_anc
    for q in range(chunks):
        piece = panel_top[:, q * width : (q + 1) * width]
        top = lax.all_gather(after(piece, earlier), "row", axis=0, tiled=True)
        earlier = top
        keep = col_keep[q * width : (q + 1) * width]
        uppers.append(product(lower_inverse, top) * keep[None, :])
        schur = product(left, top)
        parts = []
        for k in range(replicas):
            begin = partner(depth, k, replicas) * slots
            packed = place_rows(
                schur,
                lax.dynamic_slice_in_dim(row_source, begin, slots),
                lax.dynamic_slice_in_dim(row_valid, begin, slots),
            )
            if k:
                pairs = [(d, partner(d, k, replicas)) for d in range(replicas)]
                packed = lax.ppermute(packed, "depth", pairs)
            parts.append(packed)
        inside = (col_source >= q * blocks) & (col_source < (q + 1) * blocks)
        local = jnp.clip(col_source - q * blocks, 0, blocks - 1)
        total = add_columns(total, parts, local, col_valid * inside.astype(jnp.int32))
    leaf_upper = jnp.concatenate(uppers, axis=1)
    return (leaf_lower[None], leaf_upper[None], anc_lower, anc_upper, total)


def solution(mesh):
    in_specs = (
        P("depth", "row", "col"),
        P("depth", "row", "col"),
        P("depth", None, "col"),
        P("depth", "row", None),
        P("depth"),
        P("depth", "row"),
        P("depth", "col"),
        P(("row", "depth"), "col"),
        P(("row", "depth"), "col"),
        P(("row", "depth"), "col"),
        P(None, "col"),
        P(("row", "depth"), None),
    )
    out_specs = (
        P("depth", "row", "col"),
        P("depth", "row", "col"),
        P(("row", "depth"), "col"),
        P(("row", "depth"), "col"),
        P(("row", "depth"), "col"),
    )
    return jax.shard_map(shards, mesh=mesh, in_specs=in_specs, out_specs=out_specs, check_vma=False)
```
